32 devices in a mesh: facet: 4 (over z), sub: 2 (over x), base: 4 (over y, core).
Axes of the slice: x: 2, y: 2, z: 4, core: 2. Of those that a mesh axis runs over, the one named last changes fastest.
Arguments:
- sky_image: bfloat16 [16384, 1024], P(('facet', 'base')), may hold values from -6 to 6
- facet_rows: int32 [4], replicated, may hold values from 0 to 126976
- column_offset: int32 [1], replicated, may hold values from 0 to 130816
- subgrid_offsets: int32 [2], replicated, may hold values from 0 to 130816
- vis_u: int32 [2, 32768], P('sub', ('facet', 'base')), may hold values from 0 to 1023
- vis_v: int32 [2, 32768], P('sub', ('facet', 'base')), may hold values from 0 to 1023
- observed: float32 [2, 2, 32768], P('sub', None, ('facet', 'base')), may hold values from -6 to 6
- weights: float32 [2, 32768], P('sub', ('facet', 'base')), may hold values from 0.3 to 3
- block_counts: int32 [2, 16], P('sub', ('facet', 'base')), may hold values from 1 to 16
Outputs:
- residual: float32 [2, 2, 32768], P('sub', None, ('facet', 'base'))
- facet_update: bfloat16 [16384, 1024], P(('facet', 'base'), 'sub')
The draws below stay inside these ranges and needn't reach their ends.
Inputs may be any that keep to these rules, and one draw needn't show every extreme that they name: `block_counts`: the live blocks of a shard are its first ones.
All inputs are finite; a program needn't handle non-finite values.
Results may differ from the reference program's by a relative error of at most 0.008.
Values may be sent and summed in bfloat16 or wider, within the bound.
A program may use at most 64 MiB of HBM per device.

```python
import math
import jax
import jax.numpy as jnp
from jax import lax

NIMG = 131072
FS = 4096
CS = 1024
M = 256
SUBW = 1024
BLOCK = 128
VB_DEV = 16
SUBS = 2
ROWS = 16384
VIS = 32768
N_FACET = 4
N_BASE = 4


def place_ends(array, own_key, smallest, high):
    extent = array.shape
    index_at = [jax.random.randint(jax.random.fold_in(own_key, axis), (), 0, extent[axis]) for axis in range(len(extent))]
    array = array.at[tuple(index_at)].set(smallest)
    longest = extent.index(max(extent))
    index_at[longest] = (index_at[longest] + 1) % extent[longest]
    return array.at[tuple(index_at)].set(high)


def shard_levels(stream_key, shape, pieces, least, largest):
    gain, own = 1.0, jax.random.fold_in(stream_key, 6)
    for position, blocks in pieces:
        steps = jnp.exp(jax.random.uniform(jax.random.fold_in(own, position), (blocks,), jnp.float32, least / len(pieces), largest / len(pieces)))
        gain = gain * jnp.repeat(steps, shape[position] // blocks).reshape([-1 if axis == position else 1 for axis in range(len(shape))])
    return gain


def normal_values(stream_key, extent, scale, most, shards=(), kind=jnp.bfloat16):
    level = shard_levels(stream_key, extent, shards, -0.22, 0.18) if shards else 1.0
    drawn = jax.random.normal(stream_key, extent, jnp.float32) * scale * level
    return jnp.minimum(jnp.maximum(drawn, -most), most).astype(kind)


def setup_inputs(seed: int = 0) -> dict:
    streams_of = jax.random.split(jax.random.key(seed), 10)
    sky_image = normal_values(streams_of[0], (ROWS, CS), 1.0, 6.0, ((0, 16),))
    facet_rows = place_ends(jax.random.randint(streams_of[1], (N_FACET,), 0, NIMG - FS + 1), jax.random.fold_in(streams_of[1], 1), 0, NIMG - FS).astype(jnp.int32)
    column_offset = jax.random.randint(streams_of[2], (1,), 0, NIMG - M + 1).astype(jnp.int32)
    subgrid_offsets = jax.random.randint(streams_of[3], (SUBS,), 0, NIMG - M + 1).astype(jnp.int32)
    vis_u = place_ends(jax.random.randint(streams_of[4], (SUBS, VIS), 0, SUBW), jax.random.fold_in(streams_of[4], 1), 0, SUBW - 1).astype(jnp.int32)
    vis_v = place_ends(jax.random.randint(streams_of[5], (SUBS, VIS), 0, SUBW), jax.random.fold_in(streams_of[5], 1), 0, SUBW - 1).astype(jnp.int32)
    observed = normal_values(streams_of[6], (SUBS, 2, VIS), 1.0, 6.0, ((0, 2), (2, 16)), jnp.float32)
    weights = jnp.clip(jnp.exp(math.log(3.0) - 2.3025851 * jax.random.uniform(streams_of[7], (SUBS, VIS), jnp.float32) ** shard_levels(streams_of[7], (SUBS, VIS), ((0, 2), (1, 16)), -0.2, 0.2)), 0.3, 3.0)
    block_counts = place_ends(jax.random.randint(streams_of[8], (SUBS, N_FACET * N_BASE), 1, VB_DEV + 1), jax.random.fold_in(streams_of[8], 1), 1, VB_DEV).astype(jnp.int32)
    return {"sky_image": sky_image, "facet_rows": facet_rows, "column_offset": column_offset, "subgrid_offsets": subgrid_offsets, "vis_u": vis_u, "vis_v": vis_v, "observed": observed, "weights": weights, "block_counts": block_counts}


TWO_PI = 2.0 * math.pi


def modular_product(first_factor, second_factor):
    upper_part = second_factor // 256
    lower_part = second_factor % 256
    partial_mod = (first_factor * upper_part) % NIMG
    return ((partial_mod * 256) % NIMG + first_factor * lower_part) % NIMG


def phase_angle(first_factor, second_factor):
    return modular_product(first_factor, second_factor).astype(jnp.float32) * (TWO_PI / NIMG)


def grid_phase(first_factor, second_factor):
    return ((first_factor * second_factor) % SUBW).astype(jnp.float32) * (TWO_PI / SUBW)


def reference(sky_image, facet_rows, column_offset, subgrid_offsets, vis_u, vis_v, observed, weights, block_counts):
    row_ids = jnp.arange(ROWS, dtype=jnp.int32)
    row_pos = facet_rows[row_ids // FS] + row_ids % FS
    col_freq = column_offset[0] + jnp.arange(M, dtype=jnp.int32)
    col_angles = phase_angle(jnp.arange(CS, dtype=jnp.int32)[:, None], col_freq[None, :])
    col_table = (jnp.concatenate([jnp.cos(col_angles), -jnp.sin(col_angles)], axis=1) * (CS ** -0.5)).astype(jnp.bfloat16)
    spectrum = jnp.dot(sky_image, col_table, preferred_element_type=jnp.float32).astype(jnp.bfloat16)
    spectrum_rot = jnp.concatenate([spectrum[:, M:], -spectrum[:, :M]], axis=1)

    def predict(offset_row):
        frequencies = offset_row + jnp.arange(M, dtype=jnp.int32)
        angles = phase_angle(frequencies[:, None], row_pos[None, :])
        cosine = jnp.cos(angles).astype(jnp.bfloat16)
        sine_part = jnp.sin(angles).astype(jnp.bfloat16)
        summed = jnp.dot(cosine, spectrum, preferred_element_type=jnp.float32)
        summed = summed + jnp.dot(sine_part, spectrum_rot, preferred_element_type=jnp.float32)
        return (summed * (ROWS ** -0.5)).astype(jnp.bfloat16)

    subgrids = lax.map(predict, subgrid_offsets)

    shard_slots = VB_DEV * BLOCK
    slot_ids = jnp.arange(VIS, dtype=jnp.int32)
    shard_ids = slot_ids // shard_slots
    block_ids = (slot_ids % shard_slots) // BLOCK
    live_mask = block_ids[None, :] < block_counts[:, shard_ids]
    freq_ids = jnp.arange(M, dtype=jnp.int32)

    def visit_subgrid(inputs):
        grid_whole, along_u, along_v, seen_vis, weight_row, live_row = inputs
        angle_u = grid_phase(freq_ids[:, None], along_u[None, :])
        cos_along = jnp.cos(angle_u).astype(jnp.bfloat16)
        sin_along = jnp.sin(angle_u).astype(jnp.bfloat16)
        lookup = jnp.concatenate([jnp.concatenate([cos_along, -sin_along], axis=1),
                                  jnp.concatenate([sin_along, cos_along], axis=1)], axis=0)
        half_sums = jnp.dot(grid_whole, lookup, preferred_element_type=jnp.float32)
        angle_v = grid_phase(freq_ids[:, None], along_v[None, :])
        cos_rows = jnp.cos(angle_v).astype(jnp.bfloat16)
        sin_rows = jnp.sin(angle_v).astype(jnp.bfloat16)
        cos_wide = cos_rows.astype(jnp.float32)
        sin_wide = sin_rows.astype(jnp.float32)
        half_re = half_sums[:, :VIS]
        half_im = half_sums[:, VIS:]
        model_re = jnp.sum(cos_wide * half_re + sin_wide * half_im, axis=0)
        model_im = jnp.sum(cos_wide * half_im - sin_wide * half_re, axis=0)
        model_vis = jnp.stack([model_re, model_im]) * (1.0 / M)
        resid_vis = jnp.where(live_row[None, :], weight_row[None, :] * (seen_vis - model_vis), jnp.float32(0.0))
        rounded = resid_vis.astype(jnp.bfloat16).astype(jnp.float32)
        cos_cols = cos_along.astype(jnp.float32).T
        sin_cols = sin_along.astype(jnp.float32).T
        spread_re = cos_cols * rounded[0][:, None] - sin_cols * rounded[1][:, None]
        spread_im = sin_cols * rounded[0][:, None] + cos_cols * rounded[1][:, None]
        spread = jnp.concatenate([spread_re, spread_im], axis=1).astype(jnp.bfloat16)
        spread_rot = jnp.concatenate([-spread[:, M:], spread[:, :M]], axis=1)
        regrid = jnp.dot(cos_rows, spread, preferred_element_type=jnp.float32)
        regrid = regrid + jnp.dot(sin_rows, spread_rot, preferred_element_type=jnp.float32)
        return resid_vis, (regrid * (VIS ** -0.5)).astype(jnp.bfloat16)

    residual, regridded = lax.map(visit_subgrid, (subgrids, vis_u, vis_v, observed, weights, live_mask))

    def accumulate(running, inputs):
        offset_row, grid_whole = inputs
        frequencies = offset_row + jnp.arange(M, dtype=jnp.int32)
        angles = phase_angle(row_pos[:, None], frequencies[None, :])
        cosine = jnp.cos(angles).astype(jnp.bfloat16)
        sine_part = jnp.sin(angles).astype(jnp.bfloat16)
        grid_rot = jnp.concatenate([-grid_whole[:, M:], grid_whole[:, :M]], axis=1)
        running = running + jnp.dot(cosine, grid_whole, preferred_element_type=jnp.float32)
        running = running + jnp.dot(sine_part, grid_rot, preferred_element_type=jnp.float32)
        return running, None

    spectra, unused_out = lax.scan(accumulate, jnp.zeros((ROWS, 2 * M), jnp.float32), (subgrid_offsets, regridded))
    spectra = (spectra * ((SUBS * M) ** -0.5)).astype(jnp.bfloat16)
    out_angles = phase_angle(col_freq[:, None], jnp.arange(CS, dtype=jnp.int32)[None, :])
    out_table = (jnp.concatenate([jnp.cos(out_angles), -jnp.sin(out_angles)], axis=0) * (M ** -0.5)).astype(jnp.bfloat16)
    facet_update = jnp.dot(spectra, out_table, preferred_element_type=jnp.float32).astype(jnp.bfloat16)
    return residual, facet_update
```

```python
import functools
import math

import jax
import jax.numpy as jnp
from jax import lax
from jax.experimental import pallas as pl
from jax.experimental.pallas import tpu as pltpu
from jax.sharding import PartitionSpec as P

NIMG = 131072
M = 256
SUBW = 1024
BLOCK = 128
MESH = pl.DeviceIdType.MESH
F32 = jnp.float32
BF16 = jnp.bfloat16


def unit(first, second, period):
    half = period // 2
    turn = ((first * second + half) & (period - 1)) - half
    y = turn.astype(F32) * (math.pi / period)
    q = y * y
    s = F32(-1.0 / 39916800.0)
    for k in (362880.0, -5040.0, 120.0, -6.0):
        s = s * q + F32(1.0 / k)
    s = (s * q + F32(1.0)) * y
    c = F32(1.0 / 479001600.0)
    for k in (-3628800.0, 40320.0, -720.0, 24.0, -2.0):
        c = c * q + F32(1.0 / k)
    c = c * q + F32(1.0)
    return F32(1.0) - F32(2.0) * s * s, F32(2.0) * s * c


def rows_iota(count, step=1):
    return lax.broadcasted_iota(jnp.int32, (count, 1), 0) * step


def lanes_iota(count):
    return lax.broadcasted_iota(jnp.int32, (1, count), 1)


def phase_product(coarse, fine, put):
    coarse_cos, coarse_sin = coarse
    fine_cos, fine_sin = fine
    for a in range(coarse_cos.shape[0]):
        ca, sa = coarse_cos[a : a + 1, :], coarse_sin[a : a + 1, :]
        put(a, ca * fine_cos - sa * fine_sin, sa * fine_cos + ca * fine_sin)


def pieces(groups, cols):
    row_blocks = min(groups, M // 16)
    col_blocks = groups // row_blocks
    height, width = M // row_blocks, cols // col_blocks
    return [
        (r * col_blocks + c, r * height, c * width, height, width)
        for r in range(row_blocks)
        for c in range(col_blocks)
    ]


def kernel(
    sizes,
    facet_rows,
    column_offset,
    subgrid_offsets,
    counts,
    sky_hbm,
    vis_u,
    vis_v,
    observed,
    weights,
    residual_out,
    update_out,
    sky,
    t1,
    spec,
    t2,
    du,
    dv,
    t5,
    t6,
    lhs,
    acc,
    zed,
    s_a,
    r_a,
    r_b,
    s_c,
    r_c,
    r_d,
    sky_sem,
    send_sem,
    recv_sem,
):
    n_facet, n_sub, n_base = sizes
    groups = n_facet * n_base
    total = groups * n_sub
    rows, columns = sky.shape
    vis = vis_u.shape[1]
    local_cols = update_out.shape[1]
    facet, sub, base = lax.axis_index("facet"), lax.axis_index("sub"), lax.axis_index("base")
    me = facet * n_base + base
    everyone = sub * groups + me

    def member(index):
        return {"facet": index // n_base, "sub": sub, "base": lax.rem(index, n_base)}

    def anyone(index):
        inside = lax.rem(index, groups)
        return {
            "facet": inside // n_base,
            "sub": index // groups,
            "base": lax.rem(inside, n_base),
        }

    fetch = pltpu.make_async_copy(sky_hbm, sky, sky_sem)
    fetch.start()
    barrier = pltpu.get_barrier_semaphore()

    @pl.loop(1, total)
    def _(j):
        pl.semaphore_signal(
            barrier,
            inc=1,
            device_id=anyone(lax.rem(everyone + j, total)),
            device_id_type=MESH,
        )

    def wait_all(phase, buffer, count):
        whole = buffer.at[pl.ds(0, count)]
        done = pltpu.make_async_remote_copy(
            whole, whole, send_sem.at[phase], recv_sem.at[phase], member(me), MESH
        )
        done.wait_recv()
        done.wait_send()

    def scatter(phase, source, landing):
        @pl.loop(1, groups)
        def _(j):
            other = lax.rem(me + j, groups)
            pltpu.make_async_remote_copy(
                source.at[other],
                landing.at[me],
                send_sem.at[phase],
                recv_sem.at[phase],
                member(other),
                MESH,
            ).start()

        landing[me] = source[me]

    def gather(phase, buffer, slot, own, count, where):
        @pl.loop(1, count)
        def _(j):
            pltpu.make_async_remote_copy(
                buffer.at[slot],
                buffer.at[slot],
                send_sem.at[phase],
                recv_sem.at[phase],
                where(lax.rem(own + j, count)),
                MESH,
            ).start()

    def summed(landing):
        result = landing[0].astype(F32)
        for g in range(1, groups):
            result = result + landing[g].astype(F32)
        return result

    freq = column_offset[0] + lanes_iota(M)
    high = 128
    coarse = unit(rows_iota(columns // high, high), freq, NIMG)
    fine = unit(rows_iota(high), freq, NIMG)
    norm = F32(columns ** (-0.5))

    def put_t1(a, c, s):
        t1[a * high : (a + 1) * high, :M] = (c * norm).astype(BF16)
        t1[a * high : (a + 1) * high, M:] = (s * -norm).astype(BF16)

    phase_product(coarse, fine, put_t1)

    row_start = facet_rows[facet] + base * rows
    positions = row_start + lanes_iota(rows)
    own_offset = subgrid_offsets[sub]
    step = 32
    coarse = unit(own_offset + rows_iota(M // step, step), positions, NIMG)
    fine = unit(rows_iota(step), positions, NIMG)

    def put_t2(a, c, s):
        t2[a * step : (a + 1) * step, :rows] = c.astype(BF16)
        t2[a * step : (a + 1) * step, rows:] = s.astype(BF16)

    phase_product(coarse, fine, put_t2)
    fetch.wait()

    tile = min(256, rows)

    @pl.loop(0, rows // tile)
    def _(i):
        here = pl.ds(pl.multiple_of(i * tile, tile), tile)
        there = pl.ds(pl.multiple_of(rows + i * tile, tile), tile)
        part = jnp.dot(sky[here, :], t1[...], preferred_element_type=F32)
        real, imag = part[:, :M].astype(BF16), part[:, M:].astype(BF16)
        spec[here, :M] = real
        spec[here, M:] = imag
        spec[there, :M] = imag
        spec[there, M:] = -real

    def split(source, target, scale):
        blocks = pieces(groups, 2 * M)
        for g, r, c, height, width in blocks:
            target[g] = (source[r : r + height, c : c + width] * scale).astype(BF16)

    acc[:M, :] = jnp.dot(t2[...], spec[...], preferred_element_type=F32)
    split(acc, s_a, F32((rows * groups) ** (-0.5)))

    pl.semaphore_wait(barrier, total - 1)
    scatter(0, s_a, r_a)

    fan = 16

    def grid_table(position, table):
        width = 512
        for at in range(0, vis, width):
            lanes = slice(at, at + width)
            place = position[0:1, lanes]
            coarse = unit(rows_iota(M // fan, fan), place, SUBW)
            fine = unit(rows_iota(fan), place, SUBW)

            def put(a, c, s):
                table[a * fan : (a + 1) * fan, lanes] = c.astype(BF16)
                table[M + a * fan : M + (a + 1) * fan, lanes] = s.astype(BF16)

            phase_product(coarse, fine, put)

    grid_table(vis_u, du)
    wait_all(0, r_a, groups - 1)
    r_b[me] = summed(r_a).astype(BF16)
    gather(1, r_b, me, me, groups, member)
    grid_table(vis_v, dv)
    wait_all(1, r_b, groups - 1)

    for g, r, c, height, width in pieces(groups, 2 * M):
        block = r_b[g]
        part = min(width, M)
        for inner in range(0, width, part):
            value = block[:, inner : inner + part]
            at = c + inner
            lhs[r : r + height, at : at + part] = value
            if at < M:
                lhs[M + r : M + r + height, M + at : M + at + part] = -value
            else:
                lhs[M + r : M + r + height, at - M : at - M + part] = value

    chunk = 512
    acc[...] = jnp.zeros_like(acc)
    live = counts[0, 0] * BLOCK

    @pl.loop(0, vis // chunk)
    def _(i):
        lanes = pl.ds(pl.multiple_of(i * chunk, chunk), chunk)
        half = jnp.dot(lhs[...], du[:, lanes], preferred_element_type=F32)
        half_re, half_im = half[:M], half[M:]
        cos_v, sin_v = dv[:M, lanes].astype(F32), dv[M:, lanes].astype(F32)
        model_re = jnp.sum(cos_v * half_re + sin_v * half_im, axis=0, keepdims=True)
        model_im = jnp.sum(cos_v * half_im - sin_v * half_re, axis=0, keepdims=True)
        alive = lanes_iota(chunk) + i * chunk < live
        weight = weights[0:1, lanes]
        inv = F32(1.0 / M)
        res_re = jnp.where(alive, weight * (observed[0, 0:1, lanes] - model_re * inv), F32(0.0))
        res_im = jnp.where(alive, weight * (observed[0, 1:2, lanes] - model_im * inv), F32(0.0))
        residual_out[0, 0:1, lanes] = res_re
        residual_out[0, 1:2, lanes] = res_im
        r0 = res_re.astype(BF16).astype(F32)
        r1 = res_im.astype(BF16).astype(F32)
        cos_u, sin_u = du[:M, lanes].astype(F32), du[M:, lanes].astype(F32)
        spread = jnp.concatenate(
            [(cos_u * r0 - sin_u * r1).astype(BF16), (sin_u * r0 + cos_u * r1).astype(BF16)],
            axis=0,
        )
        acc[...] += lax.dot_general(
            dv[:, lanes], spread, (((1,), (1,)), ((), ())), preferred_element_type=F32
        )

    acc[:M, :M] = acc[:M, :M] - acc[M:, M:]
    acc[:M, M:] = acc[:M, M:] + acc[M:, :M]
    split(acc, s_c, F32((vis * groups) ** (-0.5)))
    scatter(2, s_c, r_c)

    for s in range(n_sub):
        freqs = subgrid_offsets[s] + lanes_iota(M)
        coarse = unit(row_start + rows_iota(rows // high, high), freqs, NIMG)
        fine = unit(rows_iota(high), freqs, NIMG)

        def put_t5(a, c, sine, at=2 * M * s):
            t5[a * high : (a + 1) * high, at : at + M] = c.astype(BF16)
            t5[a * high : (a + 1) * high, at + M : at + 2 * M] = sine.astype(BF16)

        phase_product(coarse, fine, put_t5)

    wait_all(2, r_c, groups - 1)
    r_d[everyone] = summed(r_c).astype(BF16)
    gather(3, r_d, everyone, everyone, total, anyone)

    out_cols = sub * local_cols + lanes_iota(local_cols)
    coarse = unit(column_offset[0] + rows_iota(M // step, step), out_cols, NIMG)
    fine = unit(rows_iota(step), out_cols, NIMG)
    out_norm = F32(M ** (-0.5))

    def put_t6(a, c, s):
        t6[a * step : (a + 1) * step, :] = (c * out_norm).astype(BF16)
        t6[M + a * step : M + (a + 1) * step, :] = (s * -out_norm).astype(BF16)

    phase_product(coarse, fine, put_t6)
    wait_all(3, r_d, total - 1)

    for s in range(n_sub):
        top = 2 * M * s
        for g, r, c, height, width in pieces(groups, 2 * M):
            block = r_d[s * groups + g]
            part = min(width, M)
            for inner in range(0, width, part):
                value = block[:, inner : inner + part]
                at = c + inner
                zed[top + r : top + r + height, at : at + part] = value
                low = top + M + r
                if at < M:
                    zed[low : low + height, M + at : M + at + part] = value
                else:
                    zed[low : low + height, at - M : at - M + part] = -value

    scale = F32((n_sub * M) ** (-0.5))

    @pl.loop(0, rows // tile)
    def _(i):
        here = pl.ds(pl.multiple_of(i * tile, tile), tile)
        part = jnp.dot(t5[here, :], zed[...], preferred_element_type=F32)
        share = (part * scale).astype(BF16)
        update_out[here, :] = jnp.dot(share, t6[...], preferred_element_type=F32).astype(BF16)


def shards(
    sizes,
    sky_image,
    facet_rows,
    column_offset,
    subgrid_offsets,
    vis_u,
    vis_v,
    observed,
    weights,
    block_counts,
):
    n_facet, n_sub, n_base = sizes
    groups = n_facet * n_base
    rows, columns = sky_image.shape
    vis = vis_u.shape[1]
    local_cols = columns // n_sub
    _, _, _, height, width = pieces(groups, 2 * M)[0]
    smem = pl.BlockSpec(memory_space=pltpu.SMEM)
    vmem = pl.BlockSpec(memory_space=pltpu.VMEM)
    block = (groups, height, width)
    return pl.pallas_call(
        functools.partial(kernel, sizes),
        out_shape=(
            jax.ShapeDtypeStruct(observed.shape, F32),
            jax.ShapeDtypeStruct((rows, local_cols), BF16),
        ),
        in_specs=[smem] * 4 + [pl.BlockSpec(memory_space=pl.ANY)] + [vmem] * 4,
        out_specs=(vmem, vmem),
        scratch_shapes=[
            pltpu.VMEM((rows, columns), BF16),
            pltpu.VMEM((columns, 2 * M), BF16),
            pltpu.VMEM((2 * rows, 2 * M), BF16),
            pltpu.VMEM((M, 2 * rows), BF16),
            pltpu.VMEM((2 * M, vis), BF16),
            pltpu.VMEM((2 * M, vis), BF16),
            pltpu.VMEM((rows, 2 * M * n_sub), BF16),
            pltpu.VMEM((2 * M, local_cols), BF16),
            pltpu.VMEM((2 * M, 2 * M), BF16),
            pltpu.VMEM((2 * M, 2 * M), F32),
            pltpu.VMEM((2 * M * n_sub, 2 * M), BF16),
            pltpu.VMEM(block, BF16),
            pltpu.VMEM(block, BF16),
            pltpu.VMEM(block, BF16),
            pltpu.VMEM(block, BF16),
            pltpu.VMEM(block, BF16),
            pltpu.VMEM((n_sub * groups, height, width), BF16),
            pltpu.SemaphoreType.DMA,
            pltpu.SemaphoreType.DMA((4,)),
            pltpu.SemaphoreType.DMA((4,)),
        ],
        compiler_params=pltpu.CompilerParams(
            collective_id=0, has_side_effects=True, vmem_limit_bytes=56 * 1024 * 1024
        ),
        name="column",
    )(
        facet_rows,
        column_offset,
        subgrid_offsets,
        block_counts,
        sky_image,
        vis_u,
        vis_v,
        observed,
        weights,
    )


def solution(mesh):
    sizes = (mesh.shape["facet"], mesh.shape["sub"], mesh.shape["base"])
    return jax.shard_map(
        functools.partial(shards, sizes),
        mesh=mesh,
        in_specs=(
            P(("facet", "base"), None),
            P(),
            P(),
            P(),
            P("sub", ("facet", "base")),
            P("sub", ("facet", "base")),
            P("sub", None, ("facet", "base")),
            P("sub", ("facet", "base")),
            P("sub", ("facet", "base")),
        ),
        out_specs=(P("sub", None, ("facet", "base")), P(("facet", "base"), "sub")),
        check_vma=False,
    )
```

```python
import functools
import math

import jax
import jax.numpy as jnp
from jax import lax
from jax.experimental import pallas as pl
from jax.experimental.pallas import tpu as pltpu
from jax.sharding import PartitionSpec as P

NIMG = 131072
M = 256
SUBW = 1024
BLOCK = 128
MESH = pl.DeviceIdType.MESH
F32 = jnp.float32
BF16 = jnp.bfloat16


def unit(first, second, period):
    half = period // 2
    turn = ((first * second + half) & (period - 1)) - half
    y = turn.astype(F32) * (math.pi / period)
    q = y * y
    s = F32(-1.0 / 39916800.0)
    for k in (362880.0, -5040.0, 120.0, -6.0):
        s = s * q + F32(1.0 / k)
    s = (s * q + F32(1.0)) * y
    c = F32(1.0 / 479001600.0)
    for k in (-3628800.0, 40320.0, -720.0, 24.0, -2.0):
        c = c * q + F32(1.0 / k)
    c = c * q + F32(1.0)
    return F32(1.0) - F32(2.0) * s * s, F32(2.0) * s * c


def rows_iota(count, step=1):
    return lax.broadcasted_iota(jnp.int32, (count, 1), 0) * step


def lanes_iota(count):
    return lax.broadcasted_iota(jnp.int32, (1, count), 1)


def phase_product(coarse, fine, put):
    coarse_cos, coarse_sin = coarse
    fine_cos, fine_sin = fine
    for a in range(coarse_cos.shape[0]):
        ca, sa = coarse_cos[a : a + 1, :], coarse_sin[a : a + 1, :]
        put(a, ca * fine_cos - sa * fine_sin, sa * fine_cos + ca * fine_sin)


def pieces(groups, cols):
    row_blocks = min(groups, M // 16)
    col_blocks = groups // row_blocks
    height, width = M // row_blocks, cols // col_blocks
    return [
        (r * col_blocks + c, r * height, c * width, height, width)
        for r in range(row_blocks)
        for c in range(col_blocks)
    ]


def kernel(
    sizes,
    facet_rows,
    column_offset,
    subgrid_offsets,
    counts,
    sky_hbm,
    vis_u,
    vis_v,
    observed,
    weights,
    residual_out,
    share_out,
    t6,
    sky,
    t1,
    spec,
    t2,
    du,
    dv,
    t5,
    lhs,
    acc,
    zed,
    s_a,
    x_a,
    r_a,
    r_b,
    s_c,
    x_c,
    r_c,
    r_d,
    sky_sem,
    send_sem,
    recv_sem,
):
    n_facet, n_sub, n_base = sizes
    groups = n_facet * n_base
    total = groups * n_sub
    rows, columns = sky.shape
    vis = vis_u.shape[1]
    local_cols = t6.shape[1]
    facet, sub, base = lax.axis_index("facet"), lax.axis_index("sub"), lax.axis_index("base")
    me = facet * n_base + base
    everyone = sub * groups + me
    pairs = n_base // 2
    half_group, half_total = groups // 2, total // 2
    parity = lax.rem(base, 2)
    pair = facet * pairs + base // 2
    pair_all = sub * half_group + pair
    sibling = {"facet": facet, "sub": sub, "base": base + 1 - 2 * parity}

    def slot_of(g):
        f, b = g // n_base, g % n_base
        return (b % 2) * half_group + f * pairs + b // 2

    def like(index):
        inside = lax.rem(index, half_group)
        return {
            "facet": inside // pairs,
            "sub": index // half_group,
            "base": lax.rem(inside, pairs) * 2 + parity,
        }

    def member(index):
        return {"facet": index // n_base, "sub": sub, "base": lax.rem(index, n_base)}

    def anyone(index):
        inside = lax.rem(index, groups)
        return {
            "facet": inside // n_base,
            "sub": index // groups,
            "base": lax.rem(inside, n_base),
        }

    fetch = pltpu.make_async_copy(sky_hbm, sky, sky_sem)
    fetch.start()
    barrier = pltpu.get_barrier_semaphore()

    @pl.loop(1, total)
    def _(j):
        pl.semaphore_signal(
            barrier,
            inc=1,
            device_id=anyone(lax.rem(everyone + j, total)),
            device_id_type=MESH,
        )

    def wait_all(phase, buffer, count):
        whole = buffer.at[pl.ds(0, count)]
        done = pltpu.make_async_remote_copy(
            whole, whole, send_sem.at[phase], recv_sem.at[phase], member(me), MESH
        )
        done.wait_recv()
        done.wait_send()

    def scatter(phase, source, extra, landing):
        theirs = source.at[pl.ds((1 - parity) * half_group, half_group)]
        swap = pltpu.make_async_remote_copy(
            theirs, extra, send_sem.at[phase + 4], recv_sem.at[phase + 4], sibling, MESH
        )
        swap.start()
        swap.wait()
        for i in range(half_group):
            at = parity * half_group + i
            joint = source[at].astype(F32) + extra[i].astype(F32)
            source[at] = joint.astype(BF16)

        @pl.loop(1, half_group)
        def _(j):
            other = lax.rem(pair + j, half_group)
            pltpu.make_async_remote_copy(
                source.at[parity * half_group + other],
                landing.at[pair],
                send_sem.at[phase],
                recv_sem.at[phase],
                like(sub * half_group + other),
                MESH,
            ).start()

        landing[pair] = source[parity * half_group + pair]

    def gather(phase, buffer, slot, own, start, count):
        @pl.loop(1, count)
        def _(j):
            pltpu.make_async_remote_copy(
                buffer.at[slot],
                buffer.at[slot],
                send_sem.at[phase],
                recv_sem.at[phase],
                like(start + lax.rem(own + j, count)),
                MESH,
            ).start()

    def hand_over(phase, buffer, count):
        wait_all(phase, buffer, count - 1)
        mine = buffer.at[pl.ds(parity * count, count)]
        relay = pltpu.make_async_remote_copy(
            mine, mine, send_sem.at[phase + 4], recv_sem.at[phase + 4], sibling, MESH
        )
        relay.start()
        relay.wait()

    def summed(landing):
        result = landing[0].astype(F32)
        for g in range(1, half_group):
            result = result + landing[g].astype(F32)
        return result

    freq = column_offset[0] + lanes_iota(M)
    high = 128
    coarse = unit(rows_iota(columns // high, high), freq, NIMG)
    fine = unit(rows_iota(high), freq, NIMG)
    norm = F32(columns ** (-0.5))

    def put_t1(a, c, s):
        t1[a * high : (a + 1) * high, :M] = (c * norm).astype(BF16)
        t1[a * high : (a + 1) * high, M:] = (s * -norm).astype(BF16)

    phase_product(coarse, fine, put_t1)

    row_start = facet_rows[facet] + base * rows
    positions = row_start + lanes_iota(rows)
    own_offset = subgrid_offsets[sub]
    step = 32
    coarse = unit(own_offset + rows_iota(M // step, step), positions, NIMG)
    fine = unit(rows_iota(step), positions, NIMG)

    def put_t2(a, c, s):
        t2[a * step : (a + 1) * step, :rows] = c.astype(BF16)
        t2[a * step : (a + 1) * step, rows:] = s.astype(BF16)

    phase_product(coarse, fine, put_t2)
    fetch.wait()

    tile = min(256, rows)

    @pl.loop(0, rows // tile)
    def _(i):
        here = pl.ds(pl.multiple_of(i * tile, tile), tile)
        there = pl.ds(pl.multiple_of(rows + i * tile, tile), tile)
        part = jnp.dot(sky[here, :], t1[...], preferred_element_type=F32)
        real, imag = part[:, :M].astype(BF16), part[:, M:].astype(BF16)
        spec[here, :M] = real
        spec[here, M:] = imag
        spec[there, :M] = imag
        spec[there, M:] = -real

    def split(source, target, scale):
        blocks = pieces(groups, 2 * M)
        for g, r, c, height, width in blocks:
            target[slot_of(g)] = (source[r : r + height, c : c + width] * scale).astype(BF16)

    acc[:M, :] = jnp.dot(t2[...], spec[...], preferred_element_type=F32)
    split(acc, s_a, F32((rows * groups) ** (-0.5)))

    pl.semaphore_wait(barrier, total - 1)
    scatter(0, s_a, x_a, r_a)

    fan = 16

    def grid_table(position, table):
        width = 512
        for at in range(0, vis, width):
            lanes = slice(at, at + width)
            place = position[0:1, lanes]
            coarse = unit(rows_iota(M // fan, fan), place, SUBW)
            fine = unit(rows_iota(fan), place, SUBW)

            def put(a, c, s):
                table[a * fan : (a + 1) * fan, lanes] = c.astype(BF16)
                table[M + a * fan : M + (a + 1) * fan, lanes] = s.astype(BF16)

            phase_product(coarse, fine, put)

    grid_table(vis_u, du)
    wait_all(0, r_a, half_group - 1)
    slot = parity * half_group + pair
    r_b[slot] = summed(r_a).astype(BF16)
    gather(1, r_b, slot, pair, sub * half_group, half_group)
    grid_table(vis_v, dv)
    hand_over(1, r_b, half_group)

    for g, r, c, height, width in pieces(groups, 2 * M):
        block = r_b[slot_of(g)]
        part = min(width, M)
        for inner in range(0, width, part):
            value = block[:, inner : inner + part]
            at = c + inner
            lhs[r : r + height, at : at + part] = value
            if at < M:
                lhs[M + r : M + r + height, M + at : M + at + part] = -value
            else:
                lhs[M + r : M + r + height, at - M : at - M + part] = value

    chunk = 512
    acc[...] = jnp.zeros_like(acc)
    live = counts[0, 0] * BLOCK

    @pl.loop(0, vis // chunk)
    def _(i):
        lanes = pl.ds(pl.multiple_of(i * chunk, chunk), chunk)
        half = jnp.dot(lhs[...], du[:, lanes], preferred_element_type=F32)
        half_re, half_im = half[:M], half[M:]
        cos_v, sin_v = dv[:M, lanes].astype(F32), dv[M:, lanes].astype(F32)
        model_re = jnp.sum(cos_v * half_re + sin_v * half_im, axis=0, keepdims=True)
        model_im = jnp.sum(cos_v * half_im - sin_v * half_re, axis=0, keepdims=True)
        alive = lanes_iota(chunk) + i * chunk < live
        weight = weights[0:1, lanes]
        inv = F32(1.0 / M)
        res_re = jnp.where(alive, weight * (observed[0, 0:1, lanes] - model_re * inv), F32(0.0))
        res_im = jnp.where(alive, weight * (observed[0, 1:2, lanes] - model_im * inv), F32(0.0))
        residual_out[0, 0:1, lanes] = res_re
        residual_out[0, 1:2, lanes] = res_im
        r0 = res_re.astype(BF16).astype(F32)
        r1 = res_im.astype(BF16).astype(F32)
        cos_u, sin_u = du[:M, lanes].astype(F32), du[M:, lanes].astype(F32)
        spread = jnp.concatenate(
            [(cos_u * r0 - sin_u * r1).astype(BF16), (sin_u * r0 + cos_u * r1).astype(BF16)],
            axis=0,
        )
        acc[...] += lax.dot_general(
            dv[:, lanes], spread, (((1,), (1,)), ((), ())), preferred_element_type=F32
        )

    acc[:M, :M] = acc[:M, :M] - acc[M:, M:]
    acc[:M, M:] = acc[:M, M:] + acc[M:, :M]
    split(acc, s_c, F32((vis * groups) ** (-0.5)))
    scatter(2, s_c, x_c, r_c)

    for s in range(n_sub):
        freqs = subgrid_offsets[s] + lanes_iota(M)
        coarse = unit(row_start + rows_iota(rows // high, high), freqs, NIMG)
        fine = unit(rows_iota(high), freqs, NIMG)

        def put_t5(a, c, sine, at=2 * M * s):
            t5[a * high : (a + 1) * high, at : at + M] = c.astype(BF16)
            t5[a * high : (a + 1) * high, at + M : at + 2 * M] = sine.astype(BF16)

        phase_product(coarse, fine, put_t5)

    wait_all(2, r_c, half_group - 1)
    slot_all = parity * half_total + pair_all
    r_d[slot_all] = summed(r_c).astype(BF16)
    gather(3, r_d, slot_all, pair_all, 0, half_total)

    out_cols = sub * local_cols + lanes_iota(local_cols)
    coarse = unit(column_offset[0] + rows_iota(M // step, step), out_cols, NIMG)
    fine = unit(rows_iota(step), out_cols, NIMG)
    out_norm = F32(M ** (-0.5))

    def put_t6(a, c, s):
        t6[a * step : (a + 1) * step, :] = (c * out_norm).astype(BF16)
        t6[M + a * step : M + (a + 1) * step, :] = (s * -out_norm).astype(BF16)

    phase_product(coarse, fine, put_t6)
    hand_over(3, r_d, half_total)

    for s in range(n_sub):
        top = 2 * M * s
        for g, r, c, height, width in pieces(groups, 2 * M):
            place = slot_of(g)
            block = r_d[(place // half_group) * half_total + s * half_group + place % half_group]
            part = min(width, M)
            for inner in range(0, width, part):
                value = block[:, inner : inner + part]
                at = c + inner
                zed[top + r : top + r + height, at : at + part] = value
                low = top + M + r
                if at < M:
                    zed[low : low + height, M + at : M + at + part] = value
                else:
                    zed[low : low + height, at - M : at - M + part] = -value

    scale = F32((n_sub * M) ** (-0.5))

    @pl.loop(0, rows // tile)
    def _(i):
        here = pl.ds(pl.multiple_of(i * tile, tile), tile)
        part = jnp.dot(t5[here, :], zed[...], preferred_element_type=F32)
        share = (part * scale).astype(BF16)
        share_out[here, :] = share


def shards(
    sizes,
    sky_image,
    facet_rows,
    column_offset,
    subgrid_offsets,
    vis_u,
    vis_v,
    observed,
    weights,
    block_counts,
):
    n_facet, n_sub, n_base = sizes
    groups = n_facet * n_base
    rows, columns = sky_image.shape
    vis = vis_u.shape[1]
    local_cols = columns // n_sub
    _, _, _, height, width = pieces(groups, 2 * M)[0]
    smem = pl.BlockSpec(memory_space=pltpu.SMEM)
    vmem = pl.BlockSpec(memory_space=pltpu.VMEM)
    block = (groups, height, width)
    half_block = (groups // 2, height, width)
    residual, share, table = pl.pallas_call(
        functools.partial(kernel, sizes),
        out_shape=(
            jax.ShapeDtypeStruct(observed.shape, F32),
            jax.ShapeDtypeStruct((rows, 2 * M), BF16),
            jax.ShapeDtypeStruct((2 * M, local_cols), BF16),
        ),
        in_specs=[smem] * 4 + [pl.BlockSpec(memory_space=pl.ANY)] + [vmem] * 4,
        out_specs=(vmem, vmem, vmem),
        scratch_shapes=[
            pltpu.VMEM((rows, columns), BF16),
            pltpu.VMEM((columns, 2 * M), BF16),
            pltpu.VMEM((2 * rows, 2 * M), BF16),
            pltpu.VMEM((M, 2 * rows), BF16),
            pltpu.VMEM((2 * M, vis), BF16),
            pltpu.VMEM((2 * M, vis), BF16),
            pltpu.VMEM((rows, 2 * M * n_sub), BF16),
            pltpu.VMEM((2 * M, 2 * M), BF16),
            pltpu.VMEM((2 * M, 2 * M), F32),
            pltpu.VMEM((2 * M * n_sub, 2 * M), BF16),
            pltpu.VMEM(block, BF16),
            pltpu.VMEM(half_block, BF16),
            pltpu.VMEM(half_block, BF16),
            pltpu.VMEM(block, BF16),
            pltpu.VMEM(block, BF16),
            pltpu.VMEM(half_block, BF16),
            pltpu.VMEM(half_block, BF16),
            pltpu.VMEM((n_sub * groups, height, width), BF16),
            pltpu.SemaphoreType.DMA,
            pltpu.SemaphoreType.DMA((8,)),
            pltpu.SemaphoreType.DMA((8,)),
        ],
        compiler_params=pltpu.CompilerParams(
            collective_id=0, has_side_effects=True, vmem_limit_bytes=56 * 1024 * 1024
        ),
        name="column",
    )(
        facet_rows,
        column_offset,
        subgrid_offsets,
        block_counts,
        sky_image,
        vis_u,
        vis_v,
        observed,
        weights,
    )
    return residual, jnp.dot(share, table, preferred_element_type=F32).astype(BF16)


def solution(mesh):
    sizes = (mesh.shape["facet"], mesh.shape["sub"], mesh.shape["base"])
    return jax.shard_map(
        functools.partial(shards, sizes),
        mesh=mesh,
        in_specs=(
            P(("facet", "base"), None),
            P(),
            P(),
            P(),
            P("sub", ("facet", "base")),
            P("sub", ("facet", "base")),
            P("sub", None, ("facet", "base")),
            P("sub", ("facet", "base")),
            P("sub", ("facet", "base")),
        ),
        out_specs=(P("sub", None, ("facet", "base")), P(("facet", "base"), "sub")),
        check_vma=False,
    )
```
